32 devices in a mesh: tm: 8 (over z, y), space: 4 (over x, core).
Axes of the slice: x: 2, y: 2, z: 4, core: 2. Of those that a mesh axis runs over, the one named last changes fastest.
Arguments:
- initial: float32 [8, 128, 128], P('space'), may hold values from -6 to 6
- start_guess: float32 [8, 8, 128, 128], P('tm', 'space'), may hold values from -6 to 6
- forcing: float32 [8, 5, 8, 128, 128], P('tm', None, 'space'), may hold values from -6 to 6
- step_size: float32 [8], P('tm'), may hold values from 0.06 to 0.16
Outputs:
- fine_values: float32 [8, 5, 8, 128, 128], P('tm', None, 'space')
The draws below stay inside these ranges and needn't reach their ends.
All inputs are finite; a program needn't handle non-finite values.
Results may differ from the reference program's by a relative error of at most 0.0001.
Values sent between devices are 32-bit elements; how exact they have to be, the bound alone decides.
A program may use at most 64 MiB of HBM per device.

```python
import math
import jax
import jax.numpy as jnp
import numpy as np
from jax import lax

NX = 128
NY = 128
NODES = 5
ITERS = 2
NTIME = 8
NZ = 8


def level_of(rng, shape, cuts, low, top_value):
    gain, own = 1.0, jax.random.fold_in(rng, 6)
    for axis_at, blocks in cuts:
        steps = jnp.exp(jax.random.uniform(jax.random.fold_in(own, axis_at), (blocks,), jnp.float32, low / len(cuts), top_value / len(cuts)))
        gain = gain * jnp.repeat(steps, shape[axis_at] // blocks).reshape([-1 if axis == axis_at else 1 for axis in range(len(shape))])
    return gain


def centred(stream_key, shape, scale, bound, shards=(), kind=jnp.bfloat16):
    result = scale * jax.random.normal(stream_key, shape, jnp.float32)
    if shards:
        result = result * level_of(stream_key, shape, shards, -0.22, 0.18)
    return jnp.clip(result, -bound, bound).astype(kind)


def setup_inputs(seed: int = 0) -> dict:
    arg_keys = jax.random.split(jax.random.key(seed), 5)
    return {
        "initial": centred(arg_keys[0], (NZ, NX, NY), 1.0, 6.0, ((0, 4),), jnp.float32),
        "start_guess": centred(arg_keys[1], (NTIME, NZ, NX, NY), 1.0, 6.0, ((0, 8), (1, 4)), jnp.float32),
        "forcing": centred(arg_keys[2], (NTIME, NODES, NZ, NX, NY), 1.0, 6.0, ((0, 8), (2, 4)), jnp.float32),
        "step_size": jnp.clip(jnp.exp(math.log(0.16) - 0.98082925 * jax.random.uniform(arg_keys[3], (NTIME,), jnp.float32) ** level_of(arg_keys[3], (NTIME,), ((0, 8),), -0.2, 0.2)), 0.06, 0.16),
    }


def node_tables():
    radical = math.sqrt(3.0 / 7.0)
    node_times = [0.0, (1.0 - radical) / 2.0, 0.5, (1.0 + radical) / 2.0, 1.0]
    integrals = np.zeros((4, 5))
    for column in range(5):
        coeffs = [1.0]
        for other_index in range(5):
            if other_index == column:
                continue
            other_time = node_times[other_index]
            scaling = node_times[column] - other_time
            grown = [0.0] * (len(coeffs) + 1)
            for exponent in range(len(coeffs)):
                grown[exponent + 1] += coeffs[exponent] / scaling
                grown[exponent] -= coeffs[exponent] * other_time / scaling
            coeffs = grown
        for section in range(4):
            integrals[section, column] = sum((coeffs[exponent] * (node_times[section + 1] ** (exponent + 1) - node_times[section] ** (exponent + 1)) / (exponent + 1) for exponent in range(len(coeffs))))
    coarse = [0.0, 0.5, 1.0]
    interp = np.zeros((5, 3))
    for column in range(3):
        for section in range(5):
            weight = 1.0
            for other_index in range(3):
                if other_index != column:
                    weight = weight * (node_times[section] - coarse[other_index]) / (coarse[column] - coarse[other_index])
            interp[section, column] = weight
    return (np.array(node_times), integrals, interp)

def laplace(field):
    widths = [(0, 0)] * (field.ndim - 3) + [(1, 1)] * 3
    padded = jnp.pad(field, widths)
    center = padded[..., 1:-1, 1:-1, 1:-1]
    return padded[..., 2:, 1:-1, 1:-1] + padded[..., :-2, 1:-1, 1:-1] + padded[..., 1:-1, 2:, 1:-1] + padded[..., 1:-1, :-2, 1:-1] + padded[..., 1:-1, 1:-1, 2:] + padded[..., 1:-1, 1:-1, :-2] - 6.0 * center

def fine_sweep(values, forcing, full_step, node_times, integrals):
    half_step = 0.5 * full_step
    lap_old = laplace(values)
    rates = lap_old + forcing
    swept = [values[0]]
    lap_new = [lap_old[0]]
    for section in range(4):
        quadrature = sum((float(integrals[section, column]) * rates[column] for column in range(5)))
        spacing = float(node_times[section + 1] - node_times[section])
        advanced = swept[section] + full_step * spacing * (lap_new[section] - lap_old[section]) + full_step * quadrature
        swept.append(advanced)
        lap_new.append(laplace(advanced))
    new_rates = [lap_new[column] + forcing[column] for column in range(5)]
    first_half = full_step * sum((float(integrals[0, column] + integrals[1, column]) * new_rates[column] for column in range(5)))
    second_half = full_step * sum((float(integrals[2, column] + integrals[3, column]) * new_rates[column] for column in range(5)))
    left = first_half - half_step * lap_new[0]
    right = second_half - half_step * lap_new[2]
    return (jnp.stack(swept), left, right)

def reference(initial, start_guess, forcing, step_size):
    node_times, integrals, interp = node_tables()
    values = jnp.broadcast_to(start_guess[:, None], (NTIME, NODES, NZ, NX, NY))

    def link(start_value, packed):
        left_term, right_term, half_step = packed
        middle = start_value + half_step * laplace(start_value) + left_term
        ending = middle + half_step * laplace(middle) + right_term
        return (ending, (start_value, middle, ending))
    for sweep_round in range(ITERS):
        starts = jnp.concatenate([initial[None], values[:-1, NODES - 1]], axis=0)
        values = values.at[:, 0].set(starts)
        swept, left, right = lax.map(lambda packed: fine_sweep(packed[0], packed[1], packed[2], node_times, integrals), (values, forcing, step_size))
        last_value, coarse = lax.scan(link, initial, (left, right, 0.5 * step_size))
        deltas = [coarse[0] - swept[:, 0], coarse[1] - swept[:, 2], coarse[2] - swept[:, 4]]
        values = jnp.stack([swept[:, section] + sum((float(interp[section, column]) * deltas[column] for column in range(3))) for section in range(5)], axis=1)
    return values
```

```python
import functools
import math

import jax
import jax.numpy as jnp
import numpy as np
from jax import lax
from jax.experimental import pallas as pl
from jax.experimental.pallas import tpu as pltpu
from jax.sharding import PartitionSpec as P

MESH = pl.DeviceIdType.MESH
CHUNKS = 2


def node_tables():
    radical = math.sqrt(3.0 / 7.0)
    node_times = [0.0, (1.0 - radical) / 2.0, 0.5, (1.0 + radical) / 2.0, 1.0]
    integrals = np.zeros((4, 5))
    for column in range(5):
        coeffs = [1.0]
        for other_index in range(5):
            if other_index == column:
                continue
            other_time = node_times[other_index]
            scaling = node_times[column] - other_time
            grown = [0.0] * (len(coeffs) + 1)
            for exponent in range(len(coeffs)):
                grown[exponent + 1] += coeffs[exponent] / scaling
                grown[exponent] -= coeffs[exponent] * other_time / scaling
            coeffs = grown
        for section in range(4):
            integrals[section, column] = sum(
                (
                    coeffs[exponent]
                    * (
                        node_times[section + 1] ** (exponent + 1)
                        - node_times[section] ** (exponent + 1)
                    )
                    / (exponent + 1)
                    for exponent in range(len(coeffs))
                )
            )
    coarse = [0.0, 0.5, 1.0]
    interp = np.zeros((5, 3))
    for column in range(3):
        for section in range(5):
            weight = 1.0
            for other_index in range(3):
                if other_index != column:
                    weight = (
                        weight
                        * (node_times[section] - coarse[other_index])
                        / (coarse[column] - coarse[other_index])
                    )
            interp[section, column] = weight
    return (np.array(node_times), integrals, interp)


def sine(length):
    k = np.arange(1, length + 1)
    phase = np.outer(k, k) % (2 * (length + 1))
    return math.sqrt(2.0 / (length + 1)) * np.sin(math.pi / (length + 1) * phase)


def eigen(length):
    return 2.0 - 2.0 * np.cos(math.pi / (length + 1) * np.arange(1, length + 1))


def split_pair(value):
    high = value.astype(jnp.bfloat16)
    return high, (value - high.astype(jnp.float32)).astype(jnp.bfloat16)


def dot(a, b):
    return jnp.dot(a, b, preferred_element_type=jnp.float32)


def precise(a, b):
    return dot(a[0], b[0]) + (dot(a[1], b[0]) + dot(a[0], b[1]))


def lateral(field, x_pair, y_pair):
    depth, width_x, width_y = field.shape
    mixed = precise(split_pair(field.reshape(depth * width_x, width_y)), y_pair)
    return [
        precise(x_pair, split_pair(mixed[z * width_x : (z + 1) * width_x])) for z in range(depth)
    ]


def z_sine(planes):
    count = len(planes)
    table = sine(count)
    half = (count + 1) // 2
    pairs = [
        (planes[z] + planes[count - 1 - z], planes[z] - planes[count - 1 - z])
        if z != count - 1 - z
        else (planes[z], None)
        for z in range(half)
    ]
    out = []
    for k in range(count):
        terms = [
            float(table[k, z]) * pairs[z][k % 2] for z in range(half) if pairs[z][k % 2] is not None
        ]
        total = terms[0]
        for term in terms[1:]:
            total = total + term
        out.append(total)
    return out


def weighted(weights, items):
    total = None
    for weight, item in zip(weights, items):
        weight = float(weight)
        if weight == 0.0 or item is None:
            continue
        term = item if weight == 1.0 else weight * item
        total = term if total is None else total + term
    return total


def sweep(rate, nodes, sources):
    times, integrals, _ = TABLES
    swept = [nodes[0]]
    for m in range(4):
        spacing = float(times[m + 1] - times[m])
        inner = weighted(integrals[m], nodes)
        if m > 0:
            inner = inner + spacing * (swept[m] - nodes[m])
        step = rate * inner
        if swept[m] is not None:
            step = step + swept[m]
        if sources is not None:
            step = step + sources[m]
        swept.append(step)
    first = list(integrals[0] + integrals[1])
    second = list(integrals[2] + integrals[3])
    first[0] -= 0.5
    second[2] -= 0.5
    left = rate * weighted(first, swept)
    right = rate * weighted(second, swept)
    if sources is not None:
        left = left + (sources[0] + sources[1])
        right = right + (sources[2] + sources[3])
    return swept, left, right


def corrected(swept, left, right, middle):
    interp = TABLES[2]
    ending = middle * left + right
    deltas = [None if swept[0] is None else -swept[0], left - swept[2], ending - swept[4]]
    return [
        None,
        swept[1] + weighted(interp[1], deltas),
        left,
        swept[3] + weighted(interp[3], deltas),
        ending,
    ]


def start_gains(middle):
    interp = TABLES[2]
    square = middle * middle
    return [
        None,
        float(interp[1, 0]) + float(interp[1, 1]) * middle + float(interp[1, 2]) * square,
        middle,
        float(interp[3, 0]) + float(interp[3, 1]) * middle + float(interp[3, 2]) * square,
        square,
    ]


def gains_of(rate):
    middle = 1.0 + 0.5 * rate
    gains = start_gains(middle)
    nodes = [jnp.ones_like(middle)] + gains[1:]
    swept, left, right = sweep(rate, nodes, None)
    return gains, corrected(swept, left, right, middle)


TABLES = node_tables()


def kernel(
    dims,
    step_ref, initial_hbm, guess_hbm, forcing_hbm, x_ref, y_ref, lateral_ref,
    out_hbm,
    initial, guess, forcing, result,
    in_send, in_recv, ghat, hhat, ell, own_step, steps,
    gain_c, gain_d, part_b, z_send, z_recv, own_gain, own_cross, r_send, r_recv,
    o_send, o_recv,
    load_sem, store_sem, in_ss, in_rs, h_ss, h_rs, s_ss, s_rs, z_ss, z_rs, r_ss, r_rs, o_ss, o_rs,
):
    spaces, slices, chunks, depth, length_z, rows, width_y, owners, block = dims
    me = lax.axis_index("space")
    place = lax.axis_index("tm")
    _, integrals, _ = TABLES
    width_x = spaces * chunks * rows

    load_guess = pltpu.make_async_copy(guess_hbm.at[0], guess, load_sem.at[0])
    load_forcing = pltpu.make_async_copy(forcing_hbm.at[0], forcing, load_sem.at[1])
    load_initial = pltpu.make_async_copy(initial_hbm, initial, load_sem.at[2])
    load_guess.start()
    load_forcing.start()
    load_initial.start()

    barrier = pltpu.get_barrier_semaphore()
    for i in range(1, spaces):
        pl.semaphore_signal(
            barrier, inc=1, device_id={"space": lax.rem(me + i, spaces)}, device_id_type=MESH
        )

    def greet(i, carry):
        pl.semaphore_signal(
            barrier, inc=1, device_id={"tm": lax.rem(place + i, slices)}, device_id_type=MESH
        )
        return carry

    lax.fori_loop(1, slices, greet, 0)

    step = step_ref[0]
    x_pair = (x_ref[0], x_ref[1])
    y_pair = (y_ref[0], y_ref[1])
    own_step[...] = jnp.full(own_step.shape, step, jnp.float32)
    steps[place] = jnp.full(own_step.shape, step, jnp.float32)

    def put(field, slot):
        planes = lateral(field, x_pair, y_pair)
        for target in range(spaces):
            for c in range(chunks):
                low = (target * chunks + c) * rows
                for z in range(depth):
                    in_send[c, target, slot, z] = planes[z][low : low + rows]

    def keep(c, low, high):
        in_recv[c, me, low:high] = in_send[c, me, low:high]

    groups = ((0, 1), (1, 5), (5, 6))

    def in_copy(c, group, peer, source):
        low, high = groups[group]
        return pltpu.make_async_remote_copy(
            src_ref=in_send.at[c, peer, low:high],
            dst_ref=in_recv.at[c, source, low:high],
            send_sem=in_ss.at[c, group, peer],
            recv_sem=in_rs.at[c, group, source],
            device_id={"space": peer},
            device_id_type=MESH,
        )

    def in_start(c, group):
        for i in range(1, spaces):
            in_copy(c, group, lax.rem(me + i, spaces), me).start()

    def in_wait(c, group):
        for i in range(1, spaces):
            peer = lax.rem(me + i, spaces)
            in_copy(c, group, peer, peer).wait_recv()

    load_guess.wait()
    put(guess[...], 0)
    pl.semaphore_wait(barrier, spaces - 1 + slices - 1)
    for c in range(chunks):
        in_start(c, 0)

    def step_copy(peer, source):
        return pltpu.make_async_remote_copy(
            src_ref=own_step,
            dst_ref=steps.at[source],
            send_sem=s_ss.at[peer],
            recv_sem=s_rs.at[source],
            device_id={"tm": peer},
            device_id_type=MESH,
        )

    def peers(action):
        def one(i, carry):
            action(lax.rem(place + i, slices))
            return carry

        lax.fori_loop(1, slices, one, 0)

    peers(lambda peer: step_copy(peer, place).start())

    for c in range(chunks):
        keep(c, 0, 1)
    load_forcing.wait()
    for m in range(4):
        put(step * weighted(integrals[m], [forcing[j] for j in range(5)]), m + 1)
    for c in range(chunks):
        in_start(c, 1)
        keep(c, 1, 5)
    load_initial.wait()

    @pl.when(place == 0)
    def _():
        put(initial[...], 5)
        for c in range(chunks):
            in_start(c, 2)
            keep(c, 5, 6)

    z_eigen = eigen(length_z)
    for c in range(chunks):
        low = pl.multiple_of((me * chunks + c) * rows, 8)
        base = lateral_ref[pl.ds(low, rows), :]
        for k in range(length_z):
            ell[c, k * rows : (k + 1) * rows] = -(base + float(z_eigen[k]))

    def table(i, carry):
        for c in range(chunks):
            at = pl.ds(pl.multiple_of(i * rows, 8), rows)
            gains, crossed = gains_of(step * ell[c, at])
            for m in range(1, 5):
                gain_c[c, m - 1, at] = gains[m]
                gain_d[c, m - 1, at] = crossed[m]
        return carry

    lax.fori_loop(0, length_z, table, 0)

    def planes_of(c, slot):
        return [in_recv[c, z // depth, slot, z % depth] for z in range(length_z)]

    def h_copy(c, peer):
        return pltpu.make_async_remote_copy(
            src_ref=ghat.at[c],
            dst_ref=hhat.at[c],
            send_sem=h_ss.at[c],
            recv_sem=h_rs.at[c],
            device_id={"tm": peer},
            device_id_type=MESH,
        )

    after = lax.rem(place + 1, slices)
    for c in range(chunks):
        in_wait(c, 0)
        for k, plane in enumerate(z_sine(planes_of(c, 0))):
            ghat[c, k * rows : (k + 1) * rows] = plane

        @pl.when(place < slices - 1)
        def _():
            h_copy(c, after).start()

    peers(lambda peer: step_copy(peer, peer).wait_recv())

    @pl.when(place < owners)
    def _():
        def one(p, carry):
            for c in range(chunks):
                at = pl.ds(pl.multiple_of(place * block, 8), block)
                gains, crossed = gains_of(steps[p][0:1] * ell[c, at])
                own_gain[c, p] = gains[4]
                own_cross[c, p] = crossed[4]
            return carry

        lax.fori_loop(0, slices, one, 0)

    def z_copy(c, owner, source):
        return pltpu.make_async_remote_copy(
            src_ref=z_send.at[c, owner],
            dst_ref=z_recv.at[c, source],
            send_sem=z_ss.at[c, owner],
            recv_sem=z_rs.at[c, source],
            device_id={"tm": owner},
            device_id_type=MESH,
        )

    def to_owner(owner, action):
        if owners == slices:
            action()
        else:
            pl.when(owner < owners)(action)

    first = jnp.where(place == 0, 1.0, 0.0).astype(jnp.float32)
    for c in range(chunks):
        in_wait(c, 1)
        fhat = [z_sine(planes_of(c, m + 1)) for m in range(4)]
        for m in range(4):
            for k in range(length_z):
                part_b[c, m, k * rows : (k + 1) * rows] = fhat[m][k]

        @pl.when(place == 0)
        def _():
            in_wait(c, 2)
            for k, plane in enumerate(z_sine(planes_of(c, 5))):
                hhat[c, k * rows : (k + 1) * rows] = plane

        @pl.when(place > 0)
        def _():
            h_copy(c, after).wait_recv()

        def solve(i, carry):
            at = pl.ds(pl.multiple_of(i * block, 8), block)
            rate = step * ell[c, at]
            middle = 1.0 + 0.5 * rate
            guess_hat, start = ghat[c, at], hhat[c, at]
            sources = [part_b[c, m, at] for m in range(4)]
            one = sweep(rate, [start] + [guess_hat] * 4, sources)
            nodes = corrected(*one, middle)
            rest = corrected(*sweep(rate, nodes, sources), middle)
            for m in range(1, 5):
                part_b[c, m - 1, at] = rest[m]
            seen = first * start
            gain, cross = gain_c[c, 3, at], gain_d[c, 3, at]
            z_send[c, i, 0] = nodes[4] + gain * seen
            z_send[c, i, 1] = rest[4] + (gain + cross) * seen
            return carry

        lax.fori_loop(0, owners, solve, 0)
        peers(lambda peer: to_owner(peer, lambda: z_copy(c, peer, place).start()))

        @pl.when(place < owners)
        def _():
            z_recv[c, place] = z_send[c, place]

    def r_copy(c, target, owner):
        return pltpu.make_async_remote_copy(
            src_ref=r_send.at[c, target],
            dst_ref=r_recv.at[c, owner],
            send_sem=r_ss.at[c, target],
            recv_sem=r_rs.at[c, owner],
            device_id={"tm": target},
            device_id_type=MESH,
        )

    for c in range(chunks):
        @pl.when(place < owners)
        def _():
            peers(lambda peer: z_copy(c, peer, peer).wait_recv())

            def scan(p, state):
                lower, upper = state
                r_send[c, p, 0] = lower
                r_send[c, p, 1] = upper
                gain = own_gain[c, p]
                return (
                    gain * lower + z_recv[c, p, 0],
                    gain * upper + own_cross[c, p] * lower + z_recv[c, p, 1],
                )

            zero = jnp.zeros((block, width_y), jnp.float32)
            lax.fori_loop(0, slices, scan, (zero, zero))
            peers(lambda peer: r_copy(c, peer, place).start())
            r_recv[c, place] = r_send[c, place]

    def o_copy(c, m, peer, source):
        return pltpu.make_async_remote_copy(
            src_ref=o_send.at[c, peer, m],
            dst_ref=o_recv.at[c, source, m],
            send_sem=o_ss.at[c, m, peer],
            recv_sem=o_rs.at[c, m, source],
            device_id={"space": peer},
            device_id_type=MESH,
        )

    for c in range(chunks):
        peers(lambda peer: to_owner(peer, lambda: r_copy(c, peer, peer).wait_recv()))
        own = hhat[c].reshape(owners, block, width_y)
        lower = jnp.where(place == 0, own, r_recv[c, :, 0]).reshape(length_z * rows, width_y)
        upper = jnp.where(place == 0, own, r_recv[c, :, 1]).reshape(length_z * rows, width_y)
        for m in range(5):
            if m == 0:
                value = upper
            else:
                value = (
                    gain_c[c, m - 1] * upper + gain_d[c, m - 1] * lower + part_b[c, m - 1]
                )
            planes = z_sine([value[k * rows : (k + 1) * rows] for k in range(length_z)])
            for z in range(length_z):
                o_send[c, z // depth, m, z % depth] = planes[z]
            for i in range(1, spaces):
                o_copy(c, m, lax.rem(me + i, spaces), me).start()
            o_recv[c, me, m] = o_send[c, me, m]

    def store(m):
        return pltpu.make_async_copy(result.at[m], out_hbm.at[0, m], store_sem.at[m])

    for m in range(5):
        for c in range(chunks):
            for i in range(1, spaces):
                peer = lax.rem(me + i, spaces)
                o_copy(c, m, peer, peer).wait_recv()
        field = jnp.stack(
            [
                jnp.concatenate(
                    [o_recv[c, s, m, z] for s in range(spaces) for c in range(chunks)], axis=0
                )
                for z in range(depth)
            ]
        )
        planes = lateral(field, x_pair, y_pair)
        for z in range(depth):
            result[m, z] = planes[z]
        store(m).start()

    for c in range(chunks):
        for i in range(1, spaces):
            peer = lax.rem(me + i, spaces)
            in_copy(c, 0, peer, me).wait_send()
            in_copy(c, 1, peer, me).wait_send()
            for m in range(5):
                o_copy(c, m, peer, me).wait_send()

        @pl.when(place == 0)
        def _():
            for i in range(1, spaces):
                in_copy(c, 2, lax.rem(me + i, spaces), me).wait_send()

        @pl.when(place < slices - 1)
        def _():
            h_copy(c, after).wait_send()

        peers(lambda peer: to_owner(peer, lambda: z_copy(c, peer, place).wait_send()))

        @pl.when(place < owners)
        def _():
            peers(lambda peer: r_copy(c, peer, place).wait_send())

    peers(lambda peer: step_copy(peer, place).wait_send())
    for m in range(5):
        store(m).wait()


def body(initial, start_guess, forcing, step_size):
    depth, width_x, width_y = initial.shape
    spaces, slices = lax.axis_size("space"), lax.axis_size("tm")
    length_z = depth * spaces
    chunks = CHUNKS
    rows = width_x // spaces // chunks
    owners = min(slices, length_z * rows // 8)
    block = length_z * rows // owners
    dims = (spaces, slices, chunks, depth, length_z, rows, width_y, owners, block)

    def pair(length):
        full = jnp.asarray(sine(length), jnp.float32)
        return jnp.stack(split_pair(full))

    sides = jnp.asarray(eigen(width_x)[:, None] + eigen(width_y)[None, :], jnp.float32)
    f32 = jnp.float32
    flat = length_z * rows
    dma = pltpu.SemaphoreType.DMA
    vmem = pl.BlockSpec(memory_space=pltpu.VMEM)
    hbm = pl.BlockSpec(memory_space=pl.ANY)
    return pl.pallas_call(
        functools.partial(kernel, dims),
        out_shape=jax.ShapeDtypeStruct((1, 5, depth, width_x, width_y), f32),
        in_specs=[pl.BlockSpec(memory_space=pltpu.SMEM), hbm, hbm, hbm, vmem, vmem, vmem],
        out_specs=hbm,
        scratch_shapes=[
            pltpu.VMEM((depth, width_x, width_y), f32),
            pltpu.VMEM((depth, width_x, width_y), f32),
            pltpu.VMEM((5, depth, width_x, width_y), f32),
            pltpu.VMEM((5, depth, width_x, width_y), f32),
            pltpu.VMEM((chunks, spaces, 6, depth, rows, width_y), f32),
            pltpu.VMEM((chunks, spaces, 6, depth, rows, width_y), f32),
            pltpu.VMEM((chunks, flat, width_y), f32),
            pltpu.VMEM((chunks, flat, width_y), f32),
            pltpu.VMEM((chunks, flat, width_y), f32),
            pltpu.VMEM((8, width_y), f32),
            pltpu.VMEM((slices, 8, width_y), f32),
            pltpu.VMEM((chunks, 4, flat, width_y), f32),
            pltpu.VMEM((chunks, 4, flat, width_y), f32),
            pltpu.VMEM((chunks, 4, flat, width_y), f32),
            pltpu.VMEM((chunks, owners, 2, block, width_y), f32),
            pltpu.VMEM((chunks, slices, 2, block, width_y), f32),
            pltpu.VMEM((chunks, slices, block, width_y), f32),
            pltpu.VMEM((chunks, slices, block, width_y), f32),
            pltpu.VMEM((chunks, slices, 2, block, width_y), f32),
            pltpu.VMEM((chunks, owners, 2, block, width_y), f32),
            pltpu.VMEM((chunks, spaces, 5, depth, rows, width_y), f32),
            pltpu.VMEM((chunks, spaces, 5, depth, rows, width_y), f32),
            dma((3,)),
            dma((5,)),
            dma((chunks, 3, spaces)),
            dma((chunks, 3, spaces)),
            dma((chunks,)),
            dma((chunks,)),
            dma((slices,)),
            dma((slices,)),
            dma((chunks, owners)),
            dma((chunks, slices)),
            dma((chunks, slices)),
            dma((chunks, owners)),
            dma((chunks, 5, spaces)),
            dma((chunks, 5, spaces)),
        ],
        compiler_params=pltpu.CompilerParams(collective_id=0, has_side_effects=True),
    )(step_size, initial, start_guess, forcing, pair(width_x), pair(width_y), sides)


def solution(mesh):
    in_specs = (
        P("space", None, None),
        P("tm", "space", None, None),
        P("tm", None, "space", None, None),
        P("tm"),
    )
    out_specs = P("tm", None, "space", None, None)
    return jax.shard_map(body, mesh=mesh, in_specs=in_specs, out_specs=out_specs, check_vma=False)
```

```python
import functools
import math

import jax
import jax.numpy as jnp
import numpy as np
from jax import lax
from jax.experimental import pallas as pl
from jax.experimental.pallas import tpu as pltpu
from jax.sharding import PartitionSpec as P

MESH = pl.DeviceIdType.MESH
CHUNKS = 2


def node_tables():
    radical = math.sqrt(3.0 / 7.0)
    node_times = [0.0, (1.0 - radical) / 2.0, 0.5, (1.0 + radical) / 2.0, 1.0]
    integrals = np.zeros((4, 5))
    for column in range(5):
        coeffs = [1.0]
        for other_index in range(5):
            if other_index == column:
                continue
            other_time = node_times[other_index]
            scaling = node_times[column] - other_time
            grown = [0.0] * (len(coeffs) + 1)
            for exponent in range(len(coeffs)):
                grown[exponent + 1] += coeffs[exponent] / scaling
                grown[exponent] -= coeffs[exponent] * other_time / scaling
            coeffs = grown
        for section in range(4):
            integrals[section, column] = sum(
                (
                    coeffs[exponent]
                    * (
                        node_times[section + 1] ** (exponent + 1)
                        - node_times[section] ** (exponent + 1)
                    )
                    / (exponent + 1)
                    for exponent in range(len(coeffs))
                )
            )
    coarse = [0.0, 0.5, 1.0]
    interp = np.zeros((5, 3))
    for column in range(3):
        for section in range(5):
            weight = 1.0
            for other_index in range(3):
                if other_index != column:
                    weight = (
                        weight
                        * (node_times[section] - coarse[other_index])
                        / (coarse[column] - coarse[other_index])
                    )
            interp[section, column] = weight
    return (np.array(node_times), integrals, interp)


def sine(length):
    k = np.arange(1, length + 1)
    phase = np.outer(k, k) % (2 * (length + 1))
    return math.sqrt(2.0 / (length + 1)) * np.sin(math.pi / (length + 1) * phase)


def eigen(length):
    return 2.0 - 2.0 * np.cos(math.pi / (length + 1) * np.arange(1, length + 1))


def split_pair(value):
    high = value.astype(jnp.bfloat16)
    return high, (value - high.astype(jnp.float32)).astype(jnp.bfloat16)


def dot(a, b):
    return jnp.dot(a, b, preferred_element_type=jnp.float32)


def precise(a, b):
    return dot(a[0], b[0]) + (dot(a[1], b[0]) + dot(a[0], b[1]))


def lateral(field, x_pair, y_pair):
    depth, width_x, width_y = field.shape
    mixed = precise(split_pair(field.reshape(depth * width_x, width_y)), y_pair)
    return [
        precise(x_pair, split_pair(mixed[z * width_x : (z + 1) * width_x])) for z in range(depth)
    ]


def z_sine(planes):
    count = len(planes)
    table = sine(count)
    half = (count + 1) // 2
    pairs = [
        (planes[z] + planes[count - 1 - z], planes[z] - planes[count - 1 - z])
        if z != count - 1 - z
        else (planes[z], None)
        for z in range(half)
    ]
    out = []
    for k in range(count):
        terms = [
            float(table[k, z]) * pairs[z][k % 2] for z in range(half) if pairs[z][k % 2] is not None
        ]
        total = terms[0]
        for term in terms[1:]:
            total = total + term
        out.append(total)
    return out


def weighted(weights, items):
    total = None
    for weight, item in zip(weights, items):
        weight = float(weight)
        if weight == 0.0 or item is None:
            continue
        term = item if weight == 1.0 else weight * item
        total = term if total is None else total + term
    return total


def sweep(rate, nodes, sources):
    times, integrals, _ = TABLES
    swept = [nodes[0]]
    for m in range(4):
        spacing = float(times[m + 1] - times[m])
        inner = weighted(integrals[m], nodes)
        if m > 0:
            inner = inner + spacing * (swept[m] - nodes[m])
        step = rate * inner
        if swept[m] is not None:
            step = step + swept[m]
        if sources is not None:
            step = step + sources[m]
        swept.append(step)
    first = list(integrals[0] + integrals[1])
    second = list(integrals[2] + integrals[3])
    first[0] -= 0.5
    second[2] -= 0.5
    left = rate * weighted(first, swept)
    right = rate * weighted(second, swept)
    if sources is not None:
        left = left + (sources[0] + sources[1])
        right = right + (sources[2] + sources[3])
    return swept, left, right


def corrected(swept, left, right, middle):
    interp = TABLES[2]
    ending = middle * left + right
    deltas = [None if swept[0] is None else -swept[0], left - swept[2], ending - swept[4]]
    return [
        None,
        swept[1] + weighted(interp[1], deltas),
        left,
        swept[3] + weighted(interp[3], deltas),
        ending,
    ]


def start_gains(middle):
    interp = TABLES[2]
    square = middle * middle
    return [
        None,
        float(interp[1, 0]) + float(interp[1, 1]) * middle + float(interp[1, 2]) * square,
        middle,
        float(interp[3, 0]) + float(interp[3, 1]) * middle + float(interp[3, 2]) * square,
        square,
    ]


def gains_of(rate):
    middle = 1.0 + 0.5 * rate
    gains = start_gains(middle)
    nodes = [jnp.ones_like(middle)] + gains[1:]
    swept, left, right = sweep(rate, nodes, None)
    return gains, corrected(swept, left, right, middle)


TABLES = node_tables()


def kernel(
    dims,
    step_ref, initial_hbm, guess_hbm, forcing_hbm, x_hbm, y_hbm, lateral_hbm,
    result_ref,
    initial, guess, forcing, x_ref, y_ref, lateral_ref,
    in_send, in_recv, ghat, hhat, ell, own_step, steps,
    gain_c, gain_d, part_b, z_send, z_recv, own_gain, own_cross, r_send, r_recv,
    o_send, o_recv,
    load_sem, in_ss, in_rs, h_ss, h_rs, s_ss, s_rs, z_ss, z_rs, r_ss, r_rs, o_ss, o_rs,
):
    spaces, slices, chunks, depth, length_z, rows, width_y, owners, block = dims
    me = lax.axis_index("space")
    place = lax.axis_index("tm")
    _, integrals, _ = TABLES
    width_x = spaces * chunks * rows

    barrier = pltpu.get_barrier_semaphore()
    for i in range(1, spaces):
        pl.semaphore_signal(
            barrier, inc=1, device_id={"space": lax.rem(me + i, spaces)}, device_id_type=MESH
        )

    def greet(i, carry):
        pl.semaphore_signal(
            barrier, inc=1, device_id={"tm": lax.rem(place + i, slices)}, device_id_type=MESH
        )
        return carry

    lax.fori_loop(1, slices, greet, 0)

    sources = (guess_hbm.at[0], x_hbm, y_hbm, forcing_hbm.at[0], initial_hbm, lateral_hbm)
    loads = [
        pltpu.make_async_copy(source, target, load_sem.at[i])
        for i, (source, target) in enumerate(
            zip(sources, (guess, x_ref, y_ref, forcing, initial, lateral_ref))
        )
    ]
    for load in loads:
        load.start()
    load_guess, load_x, load_y, load_forcing, load_initial, load_lateral = loads

    step = step_ref[0]
    own_step[...] = jnp.full(own_step.shape, step, jnp.float32)
    steps[place] = jnp.full(own_step.shape, step, jnp.float32)

    def put(field, slot):
        planes = lateral(field, x_pair, y_pair)
        for target in range(spaces):
            for c in range(chunks):
                low = (target * chunks + c) * rows
                for z in range(depth):
                    in_send[c, target, slot, z] = planes[z][low : low + rows]

    def keep(c, low, high):
        in_recv[c, me, low:high] = in_send[c, me, low:high]

    groups = ((0, 1), (1, 5), (5, 6))

    def in_copy(c, group, peer, source):
        low, high = groups[group]
        return pltpu.make_async_remote_copy(
            src_ref=in_send.at[c, peer, low:high],
            dst_ref=in_recv.at[c, source, low:high],
            send_sem=in_ss.at[c, group, peer],
            recv_sem=in_rs.at[c, group, source],
            device_id={"space": peer},
            device_id_type=MESH,
        )

    def in_start(c, group):
        for i in range(1, spaces):
            in_copy(c, group, lax.rem(me + i, spaces), me).start()

    def in_wait(c, group):
        for i in range(1, spaces):
            peer = lax.rem(me + i, spaces)
            in_copy(c, group, peer, peer).wait_recv()

    load_guess.wait()
    load_x.wait()
    load_y.wait()
    x_pair = (x_ref[0], x_ref[1])
    y_pair = (y_ref[0], y_ref[1])
    put(guess[...], 0)
    pl.semaphore_wait(barrier, spaces - 1 + slices - 1)
    for c in range(chunks):
        in_start(c, 0)

    def step_copy(peer, source):
        return pltpu.make_async_remote_copy(
            src_ref=own_step,
            dst_ref=steps.at[source],
            send_sem=s_ss.at[peer],
            recv_sem=s_rs.at[source],
            device_id={"tm": peer},
            device_id_type=MESH,
        )

    def peers(action):
        def one(i, carry):
            action(lax.rem(place + i, slices))
            return carry

        lax.fori_loop(1, slices, one, 0)

    peers(lambda peer: step_copy(peer, place).start())

    for c in range(chunks):
        keep(c, 0, 1)
    load_initial.wait()

    @pl.when(place == 0)
    def _():
        put(initial[...], 5)
        for c in range(chunks):
            in_start(c, 2)
            keep(c, 5, 6)

    load_forcing.wait()
    for m in range(4):
        put(step * weighted(integrals[m], [forcing[j] for j in range(5)]), m + 1)
    for c in range(chunks):
        in_start(c, 1)
        keep(c, 1, 5)
    z_eigen = eigen(length_z)
    load_lateral.wait()
    for c in range(chunks):
        low = pl.multiple_of((me * chunks + c) * rows, 8)
        base = lateral_ref[pl.ds(low, rows), :]
        for k in range(length_z):
            ell[c, k * rows : (k + 1) * rows] = -(base + float(z_eigen[k]))

    def table(i, carry):
        for c in range(chunks):
            at = pl.ds(pl.multiple_of(i * rows, 8), rows)
            gains, crossed = gains_of(step * ell[c, at])
            for m in range(1, 5):
                gain_c[c, m - 1, at] = gains[m]
                gain_d[c, m - 1, at] = crossed[m]
        return carry

    lax.fori_loop(0, length_z, table, 0)

    def planes_of(c, slot):
        return [in_recv[c, z // depth, slot, z % depth] for z in range(length_z)]

    def h_copy(c, peer):
        return pltpu.make_async_remote_copy(
            src_ref=ghat.at[c],
            dst_ref=hhat.at[c],
            send_sem=h_ss.at[c],
            recv_sem=h_rs.at[c],
            device_id={"tm": peer},
            device_id_type=MESH,
        )

    after = lax.rem(place + 1, slices)
    for c in range(chunks):
        in_wait(c, 0)
        for k, plane in enumerate(z_sine(planes_of(c, 0))):
            ghat[c, k * rows : (k + 1) * rows] = plane

        @pl.when(place < slices - 1)
        def _():
            h_copy(c, after).start()

    peers(lambda peer: step_copy(peer, peer).wait_recv())

    @pl.when(place < owners)
    def _():
        def one(p, carry):
            for c in range(chunks):
                at = pl.ds(pl.multiple_of(place * block, 8), block)
                gains, crossed = gains_of(steps[p][0:1] * ell[c, at])
                own_gain[c, p] = gains[4]
                own_cross[c, p] = crossed[4]
            return carry

        lax.fori_loop(0, slices, one, 0)

    def z_copy(c, owner, source):
        return pltpu.make_async_remote_copy(
            src_ref=z_send.at[c, owner],
            dst_ref=z_recv.at[c, source],
            send_sem=z_ss.at[c, owner],
            recv_sem=z_rs.at[c, source],
            device_id={"tm": owner},
            device_id_type=MESH,
        )

    def to_owner(owner, action):
        if owners == slices:
            action()
        else:
            pl.when(owner < owners)(action)

    first = jnp.where(place == 0, 1.0, 0.0).astype(jnp.float32)
    for c in range(chunks):
        in_wait(c, 1)
        fhat = [z_sine(planes_of(c, m + 1)) for m in range(4)]
        for m in range(4):
            for k in range(length_z):
                part_b[c, m, k * rows : (k + 1) * rows] = fhat[m][k]

        @pl.when(place == 0)
        def _():
            in_wait(c, 2)
            for k, plane in enumerate(z_sine(planes_of(c, 5))):
                hhat[c, k * rows : (k + 1) * rows] = plane

        @pl.when(place > 0)
        def _():
            h_copy(c, after).wait_recv()

        def solve(i, carry):
            at = pl.ds(pl.multiple_of(i * block, 8), block)
            rate = step * ell[c, at]
            middle = 1.0 + 0.5 * rate
            guess_hat, start = ghat[c, at], hhat[c, at]
            sources = [part_b[c, m, at] for m in range(4)]
            one = sweep(rate, [start] + [guess_hat] * 4, sources)
            nodes = corrected(*one, middle)
            rest = corrected(*sweep(rate, nodes, sources), middle)
            for m in range(1, 5):
                part_b[c, m - 1, at] = rest[m]
            seen = first * start
            gain, cross = gain_c[c, 3, at], gain_d[c, 3, at]
            z_send[c, i, 0] = nodes[4] + gain * seen
            z_send[c, i, 1] = rest[4] + (gain + cross) * seen
            return carry

        lax.fori_loop(0, owners, solve, 0)
        peers(lambda peer: to_owner(peer, lambda: z_copy(c, peer, place).start()))

        @pl.when(place < owners)
        def _():
            z_recv[c, place] = z_send[c, place]

    def r_copy(c, target, owner):
        return pltpu.make_async_remote_copy(
            src_ref=r_send.at[c, target],
            dst_ref=r_recv.at[c, owner],
            send_sem=r_ss.at[c, target],
            recv_sem=r_rs.at[c, owner],
            device_id={"tm": target},
            device_id_type=MESH,
        )

    for c in range(chunks):
        @pl.when(place < owners)
        def _():
            peers(lambda peer: z_copy(c, peer, peer).wait_recv())

            def scan(p, state):
                lower, upper = state
                r_send[c, p, 0] = lower
                r_send[c, p, 1] = upper
                gain = own_gain[c, p]
                return (
                    gain * lower + z_recv[c, p, 0],
                    gain * upper + own_cross[c, p] * lower + z_recv[c, p, 1],
                )

            zero = jnp.zeros((block, width_y), jnp.float32)
            lax.fori_loop(0, slices, scan, (zero, zero))
            peers(lambda peer: r_copy(c, peer, place).start())
            r_recv[c, place] = r_send[c, place]

    def o_groups(c):
        return ((0, 1), (1, 2), (2, 3), (3, 4), (4, 5)) if c == chunks - 1 else ((0, 5),)

    def o_copy(c, group, peer, source):
        low, high = o_groups(c)[group]
        return pltpu.make_async_remote_copy(
            src_ref=o_send.at[c, peer, low:high],
            dst_ref=o_recv.at[c, source, low:high],
            send_sem=o_ss.at[c, group, peer],
            recv_sem=o_rs.at[c, group, source],
            device_id={"space": peer},
            device_id_type=MESH,
        )

    for c in range(chunks):
        peers(lambda peer: to_owner(peer, lambda: r_copy(c, peer, peer).wait_recv()))
        own = hhat[c].reshape(owners, block, width_y)
        lower = jnp.where(place == 0, own, r_recv[c, :, 0]).reshape(length_z * rows, width_y)
        upper = jnp.where(place == 0, own, r_recv[c, :, 1]).reshape(length_z * rows, width_y)
        for m in range(5):
            if m == 0:
                value = upper
            else:
                value = (
                    gain_c[c, m - 1] * upper + gain_d[c, m - 1] * lower + part_b[c, m - 1]
                )
            planes = z_sine([value[k * rows : (k + 1) * rows] for k in range(length_z)])
            for z in range(length_z):
                o_send[c, z // depth, m, z % depth] = planes[z]
            o_recv[c, me, m] = o_send[c, me, m]
            for group, (_, high) in enumerate(o_groups(c)):
                if high == m + 1:
                    for i in range(1, spaces):
                        o_copy(c, group, lax.rem(me + i, spaces), me).start()

    for m in range(5):
        for c in range(chunks):
            for group, (low, _) in enumerate(o_groups(c)):
                if low == m:
                    for i in range(1, spaces):
                        peer = lax.rem(me + i, spaces)
                        o_copy(c, group, peer, peer).wait_recv()
        field = jnp.stack(
            [
                jnp.concatenate(
                    [o_recv[c, s, m, z] for s in range(spaces) for c in range(chunks)], axis=0
                )
                for z in range(depth)
            ]
        )
        planes = lateral(field, x_pair, y_pair)
        for z in range(depth):
            result_ref[0, m, z] = planes[z]

    for c in range(chunks):
        for i in range(1, spaces):
            peer = lax.rem(me + i, spaces)
            in_copy(c, 0, peer, me).wait_send()
            in_copy(c, 1, peer, me).wait_send()
            for group in range(len(o_groups(c))):
                o_copy(c, group, peer, me).wait_send()

        @pl.when(place == 0)
        def _():
            for i in range(1, spaces):
                in_copy(c, 2, lax.rem(me + i, spaces), me).wait_send()

        @pl.when(place < slices - 1)
        def _():
            h_copy(c, after).wait_send()

        peers(lambda peer: to_owner(peer, lambda: z_copy(c, peer, place).wait_send()))

        @pl.when(place < owners)
        def _():
            peers(lambda peer: r_copy(c, peer, place).wait_send())

    peers(lambda peer: step_copy(peer, place).wait_send())


def body(initial, start_guess, forcing, step_size):
    depth, width_x, width_y = initial.shape
    spaces, slices = lax.axis_size("space"), lax.axis_size("tm")
    length_z = depth * spaces
    chunks = CHUNKS
    rows = width_x // spaces // chunks
    owners = min(slices, length_z * rows // 8)
    block = length_z * rows // owners
    dims = (spaces, slices, chunks, depth, length_z, rows, width_y, owners, block)

    def pair(length):
        full = jnp.asarray(sine(length), jnp.float32)
        return jnp.stack(split_pair(full))

    sides = jnp.asarray(eigen(width_x)[:, None] + eigen(width_y)[None, :], jnp.float32)
    f32 = jnp.float32
    flat = length_z * rows
    dma = pltpu.SemaphoreType.DMA
    vmem = pl.BlockSpec(memory_space=pltpu.VMEM)
    hbm = pl.BlockSpec(memory_space=pl.ANY)
    return pl.pallas_call(
        functools.partial(kernel, dims),
        out_shape=pltpu.VMEM((1, 5, depth, width_x, width_y), f32),
        in_specs=[pl.BlockSpec(memory_space=pltpu.SMEM), hbm, hbm, hbm, hbm, hbm, hbm],
        out_specs=vmem,
        scratch_shapes=[
            pltpu.VMEM((depth, width_x, width_y), f32),
            pltpu.VMEM((depth, width_x, width_y), f32),
            pltpu.VMEM((5, depth, width_x, width_y), f32),
            pltpu.VMEM((2, width_x, width_x), jnp.bfloat16),
            pltpu.VMEM((2, width_y, width_y), jnp.bfloat16),
            pltpu.VMEM((width_x, width_y), f32),
            pltpu.VMEM((chunks, spaces, 6, depth, rows, width_y), f32),
            pltpu.VMEM((chunks, spaces, 6, depth, rows, width_y), f32),
            pltpu.VMEM((chunks, flat, width_y), f32),
            pltpu.VMEM((chunks, flat, width_y), f32),
            pltpu.VMEM((chunks, flat, width_y), f32),
            pltpu.VMEM((8, width_y), f32),
            pltpu.VMEM((slices, 8, width_y), f32),
            pltpu.VMEM((chunks, 4, flat, width_y), f32),
            pltpu.VMEM((chunks, 4, flat, width_y), f32),
            pltpu.VMEM((chunks, 4, flat, width_y), f32),
            pltpu.VMEM((chunks, owners, 2, block, width_y), f32),
            pltpu.VMEM((chunks, slices, 2, block, width_y), f32),
            pltpu.VMEM((chunks, slices, block, width_y), f32),
            pltpu.VMEM((chunks, slices, block, width_y), f32),
            pltpu.VMEM((chunks, slices, 2, block, width_y), f32),
            pltpu.VMEM((chunks, owners, 2, block, width_y), f32),
            pltpu.VMEM((chunks, spaces, 5, depth, rows, width_y), f32),
            pltpu.VMEM((chunks, spaces, 5, depth, rows, width_y), f32),
            dma((6,)),
            dma((chunks, 3, spaces)),
            dma((chunks, 3, spaces)),
            dma((chunks,)),
            dma((chunks,)),
            dma((slices,)),
            dma((slices,)),
            dma((chunks, owners)),
            dma((chunks, slices)),
            dma((chunks, slices)),
            dma((chunks, owners)),
            dma((chunks, 5, spaces)),
            dma((chunks, 5, spaces)),
        ],
        compiler_params=pltpu.CompilerParams(collective_id=0, has_side_effects=True),
    )(step_size, initial, start_guess, forcing, pair(width_x), pair(width_y), sides)


def solution(mesh):
    in_specs = (
        P("space", None, None),
        P("tm", "space", None, None),
        P("tm", None, "space", None, None),
        P("tm"),
    )
    out_specs = P("tm", None, "space", None, None)
    return jax.shard_map(body, mesh=mesh, in_specs=in_specs, out_specs=out_specs, check_vma=False)
```

```python
import functools
import math

import jax
import jax.numpy as jnp
import numpy as np
from jax import lax
from jax.experimental import pallas as pl
from jax.experimental.pallas import tpu as pltpu
from jax.sharding import PartitionSpec as P

MESH = pl.DeviceIdType.MESH
CHUNKS = 2


def node_tables():
    radical = math.sqrt(3.0 / 7.0)
    node_times = [0.0, (1.0 - radical) / 2.0, 0.5, (1.0 + radical) / 2.0, 1.0]
    integrals = np.zeros((4, 5))
    for column in range(5):
        coeffs = [1.0]
        for other_index in range(5):
            if other_index == column:
                continue
            other_time = node_times[other_index]
            scaling = node_times[column] - other_time
            grown = [0.0] * (len(coeffs) + 1)
            for exponent in range(len(coeffs)):
                grown[exponent + 1] += coeffs[exponent] / scaling
                grown[exponent] -= coeffs[exponent] * other_time / scaling
            coeffs = grown
        for section in range(4):
            integrals[section, column] = sum(
                (
                    coeffs[exponent]
                    * (
                        node_times[section + 1] ** (exponent + 1)
                        - node_times[section] ** (exponent + 1)
                    )
                    / (exponent + 1)
                    for exponent in range(len(coeffs))
                )
            )
    coarse = [0.0, 0.5, 1.0]
    interp = np.zeros((5, 3))
    for column in range(3):
        for section in range(5):
            weight = 1.0
            for other_index in range(3):
                if other_index != column:
                    weight = (
                        weight
                        * (node_times[section] - coarse[other_index])
                        / (coarse[column] - coarse[other_index])
                    )
            interp[section, column] = weight
    return (np.array(node_times), integrals, interp)


def sine(length):
    k = np.arange(1, length + 1)
    phase = np.outer(k, k) % (2 * (length + 1))
    return math.sqrt(2.0 / (length + 1)) * np.sin(math.pi / (length + 1) * phase)


def eigen(length):
    return 2.0 - 2.0 * np.cos(math.pi / (length + 1) * np.arange(1, length + 1))


def split_pair(value):
    high = value.astype(jnp.bfloat16)
    return high, (value - high.astype(jnp.float32)).astype(jnp.bfloat16)


def dot(a, b):
    return jnp.dot(a, b, preferred_element_type=jnp.float32)


def precise(a, b):
    return dot(a[0], b[0]) + (dot(a[1], b[0]) + dot(a[0], b[1]))


def lateral(field, x_pair, y_pair):
    depth, width_x, width_y = field.shape
    mixed = precise(split_pair(field.reshape(depth * width_x, width_y)), y_pair)
    return [
        precise(x_pair, split_pair(mixed[z * width_x : (z + 1) * width_x])) for z in range(depth)
    ]


def z_sine(planes):
    count = len(planes)
    table = sine(count)
    half = (count + 1) // 2
    pairs = [
        (planes[z] + planes[count - 1 - z], planes[z] - planes[count - 1 - z])
        if z != count - 1 - z
        else (planes[z], None)
        for z in range(half)
    ]
    out = []
    for k in range(count):
        terms = [
            float(table[k, z]) * pairs[z][k % 2] for z in range(half) if pairs[z][k % 2] is not None
        ]
        total = terms[0]
        for term in terms[1:]:
            total = total + term
        out.append(total)
    return out


def weighted(weights, items):
    total = None
    for weight, item in zip(weights, items):
        weight = float(weight)
        if weight == 0.0 or item is None:
            continue
        term = item if weight == 1.0 else weight * item
        total = term if total is None else total + term
    return total


def sweep(rate, nodes, sources):
    times, integrals, _ = TABLES
    swept = [nodes[0]]
    for m in range(4):
        spacing = float(times[m + 1] - times[m])
        inner = weighted(integrals[m], nodes)
        if m > 0:
            inner = inner + spacing * (swept[m] - nodes[m])
        step = rate * inner
        if swept[m] is not None:
            step = step + swept[m]
        if sources is not None:
            step = step + sources[m]
        swept.append(step)
    first = list(integrals[0] + integrals[1])
    second = list(integrals[2] + integrals[3])
    first[0] -= 0.5
    second[2] -= 0.5
    left = rate * weighted(first, swept)
    right = rate * weighted(second, swept)
    if sources is not None:
        left = left + (sources[0] + sources[1])
        right = right + (sources[2] + sources[3])
    return swept, left, right


def corrected(swept, left, right, middle):
    interp = TABLES[2]
    ending = middle * left + right
    deltas = [None if swept[0] is None else -swept[0], left - swept[2], ending - swept[4]]
    return [
        None,
        swept[1] + weighted(interp[1], deltas),
        left,
        swept[3] + weighted(interp[3], deltas),
        ending,
    ]


def start_gains(middle):
    interp = TABLES[2]
    square = middle * middle
    return [
        None,
        float(interp[1, 0]) + float(interp[1, 1]) * middle + float(interp[1, 2]) * square,
        middle,
        float(interp[3, 0]) + float(interp[3, 1]) * middle + float(interp[3, 2]) * square,
        square,
    ]


def gains_of(rate):
    middle = 1.0 + 0.5 * rate
    gains = start_gains(middle)
    nodes = [jnp.ones_like(middle)] + gains[1:]
    swept, left, right = sweep(rate, nodes, None)
    return gains, corrected(swept, left, right, middle)


TABLES = node_tables()


def kernel(
    dims,
    step_ref, initial_hbm, guess_hbm, forcing_hbm, x_hbm, y_hbm, lateral_hbm,
    result_ref,
    initial, guess, forcing, x_ref, y_ref, lateral_ref,
    in_send, in_recv, ghat, hhat, ell, own_step, steps,
    gain_c, gain_d, part_b, z_send, z_recv, own_gain, own_cross, r_send, r_recv,
    o_send, o_recv,
    load_sem, in_ss, in_rs, h_ss, h_rs, s_ss, s_rs, z_ss, z_rs, r_ss, r_rs, o_ss, o_rs,
):
    spaces, slices, chunks, depth, length_z, rows, width_y, owners, block = dims
    me = lax.axis_index("space")
    place = lax.axis_index("tm")
    _, integrals, _ = TABLES
    width_x = spaces * chunks * rows

    barrier = pltpu.get_barrier_semaphore()
    for i in range(1, spaces):
        pl.semaphore_signal(
            barrier, inc=1, device_id={"space": lax.rem(me + i, spaces)}, device_id_type=MESH
        )

    def greet(i, carry):
        pl.semaphore_signal(
            barrier, inc=1, device_id={"tm": lax.rem(place + i, slices)}, device_id_type=MESH
        )
        return carry

    lax.fori_loop(1, slices, greet, 0)

    sources = (guess_hbm.at[0], x_hbm, y_hbm, forcing_hbm.at[0], initial_hbm, lateral_hbm)
    loads = [
        pltpu.make_async_copy(source, target, load_sem.at[i])
        for i, (source, target) in enumerate(
            zip(sources, (guess, x_ref, y_ref, forcing, initial, lateral_ref))
        )
    ]
    for load in loads:
        load.start()
    load_guess, load_x, load_y, load_forcing, load_initial, load_lateral = loads

    step = step_ref[0]
    own_step[...] = jnp.full(own_step.shape, step, jnp.float32)
    steps[place] = jnp.full(own_step.shape, step, jnp.float32)

    def put(field, slot):
        planes = lateral(field, x_pair, y_pair)
        for target in range(spaces):
            for c in range(chunks):
                low = (target * chunks + c) * rows
                for z in range(depth):
                    in_send[c, target, slot, z] = planes[z][low : low + rows]

    def keep(c, low, high):
        in_recv[c, me, low:high] = in_send[c, me, low:high]

    groups = ((0, 1), (1, 5), (5, 6))

    def in_copy(c, group, peer, source):
        low, high = groups[group]
        return pltpu.make_async_remote_copy(
            src_ref=in_send.at[c, peer, low:high],
            dst_ref=in_recv.at[c, source, low:high],
            send_sem=in_ss.at[c, group, peer],
            recv_sem=in_rs.at[c, group, source],
            device_id={"space": peer},
            device_id_type=MESH,
        )

    def in_start(c, group):
        for i in range(1, spaces):
            in_copy(c, group, lax.rem(me + i, spaces), me).start()

    def in_wait(c, group):
        for i in range(1, spaces):
            peer = lax.rem(me + i, spaces)
            in_copy(c, group, peer, peer).wait_recv()

    load_guess.wait()
    load_x.wait()
    load_y.wait()
    x_pair = (x_ref[0], x_ref[1])
    y_pair = (y_ref[0], y_ref[1])
    put(guess[...], 0)
    pl.semaphore_wait(barrier, spaces - 1 + slices - 1)
    for c in range(chunks):
        in_start(c, 0)

    def step_copy(peer, source):
        return pltpu.make_async_remote_copy(
            src_ref=own_step,
            dst_ref=steps.at[source],
            send_sem=s_ss.at[peer],
            recv_sem=s_rs.at[source],
            device_id={"tm": peer},
            device_id_type=MESH,
        )

    def peers(action):
        def one(i, carry):
            action(lax.rem(place + i, slices))
            return carry

        if slices > 8:
            lax.fori_loop(1, slices, one, 0)
        else:
            for i in range(1, slices):
                one(i, 0)

    peers(lambda peer: step_copy(peer, place).start())

    for c in range(chunks):
        keep(c, 0, 1)
    load_initial.wait()

    @pl.when(place == 0)
    def _():
        put(initial[...], 5)
        for c in range(chunks):
            in_start(c, 2)
            keep(c, 5, 6)

    load_forcing.wait()
    for m in range(4):
        put(step * weighted(integrals[m], [forcing[j] for j in range(5)]), m + 1)
    for c in range(chunks):
        in_start(c, 1)
        keep(c, 1, 5)
    z_eigen = eigen(length_z)
    load_lateral.wait()
    for c in range(chunks):
        low = pl.multiple_of((me * chunks + c) * rows, 8)
        base = lateral_ref[pl.ds(low, rows), :]
        for k in range(length_z):
            ell[c, k * rows : (k + 1) * rows] = -(base + float(z_eigen[k]))

    def table(i, carry):
        for c in range(chunks):
            at = pl.ds(pl.multiple_of(i * rows, 8), rows)
            gains, crossed = gains_of(step * ell[c, at])
            for m in range(1, 5):
                gain_c[c, m - 1, at] = gains[m]
                gain_d[c, m - 1, at] = crossed[m]
        return carry

    lax.fori_loop(0, length_z, table, 0, unroll=2)

    def planes_of(c, slot):
        return [in_recv[c, z // depth, slot, z % depth] for z in range(length_z)]

    def h_copy(c, peer):
        return pltpu.make_async_remote_copy(
            src_ref=ghat.at[c],
            dst_ref=hhat.at[c],
            send_sem=h_ss.at[c],
            recv_sem=h_rs.at[c],
            device_id={"tm": peer},
            device_id_type=MESH,
        )

    after = lax.rem(place + 1, slices)
    for c in range(chunks):
        in_wait(c, 0)
        for k, plane in enumerate(z_sine(planes_of(c, 0))):
            ghat[c, k * rows : (k + 1) * rows] = plane

        @pl.when(place < slices - 1)
        def _():
            h_copy(c, after).start()

    peers(lambda peer: step_copy(peer, peer).wait_recv())

    @pl.when(place < owners)
    def _():
        def one(p, carry):
            for c in range(chunks):
                at = pl.ds(pl.multiple_of(place * block, 8), block)
                gains, crossed = gains_of(steps[p][0:1] * ell[c, at])
                own_gain[c, p] = gains[4]
                own_cross[c, p] = crossed[4]
            return carry

        lax.fori_loop(0, slices, one, 0, unroll=2)

    def z_copy(c, owner, source):
        return pltpu.make_async_remote_copy(
            src_ref=z_send.at[c, owner],
            dst_ref=z_recv.at[c, source],
            send_sem=z_ss.at[c],
            recv_sem=z_rs.at[c],
            device_id={"tm": owner},
            device_id_type=MESH,
        )

    def to_owner(owner, action):
        if owners == slices:
            action()
        else:
            pl.when(owner < owners)(action)

    def bulk_wait(ref, sem, count):
        pltpu.make_async_copy(ref.at[0:count], ref.at[0:count], sem).wait()

    def owner_wait(ref, sem):
        if owners == slices:
            bulk_wait(ref, sem, owners - 1)
        else:
            pl.when(place < owners)(lambda: bulk_wait(ref, sem, owners - 1))
            pl.when(place >= owners)(lambda: bulk_wait(ref, sem, owners))

    first = jnp.where(place == 0, 1.0, 0.0).astype(jnp.float32)
    for c in range(chunks):
        in_wait(c, 1)
        fhat = [z_sine(planes_of(c, m + 1)) for m in range(4)]
        for m in range(4):
            for k in range(length_z):
                part_b[c, m, k * rows : (k + 1) * rows] = fhat[m][k]

        @pl.when(place == 0)
        def _():
            in_wait(c, 2)
            for k, plane in enumerate(z_sine(planes_of(c, 5))):
                hhat[c, k * rows : (k + 1) * rows] = plane

        @pl.when(place > 0)
        def _():
            h_copy(c, after).wait_recv()

        def solve(i, carry):
            at = pl.ds(pl.multiple_of(i * block, 8), block)
            rate = step * ell[c, at]
            middle = 1.0 + 0.5 * rate
            guess_hat, start = ghat[c, at], hhat[c, at]
            sources = [part_b[c, m, at] for m in range(4)]
            one = sweep(rate, [start] + [guess_hat] * 4, sources)
            nodes = corrected(*one, middle)
            rest = corrected(*sweep(rate, nodes, sources), middle)
            for m in range(1, 5):
                part_b[c, m - 1, at] = rest[m]
            seen = first * start
            gain, cross = gain_c[c, 3, at], gain_d[c, 3, at]
            z_send[c, i, 0] = nodes[4] + gain * seen
            z_send[c, i, 1] = rest[4] + (gain + cross) * seen
            return carry

        lax.fori_loop(0, owners, solve, 0, unroll=4)
        peers(lambda peer: to_owner(peer, lambda: z_copy(c, peer, place).start()))

        @pl.when(place < owners)
        def _():
            z_recv[c, place] = z_send[c, place]

    def r_copy(c, target, owner):
        return pltpu.make_async_remote_copy(
            src_ref=r_send.at[c, target],
            dst_ref=r_recv.at[c, owner],
            send_sem=r_ss.at[c],
            recv_sem=r_rs.at[c],
            device_id={"tm": target},
            device_id_type=MESH,
        )

    for c in range(chunks):
        @pl.when(place < owners)
        def _():
            bulk_wait(z_recv.at[c], z_rs.at[c], slices - 1)

            def scan(p, state):
                lower, upper = state
                r_send[c, p, 0] = lower
                r_send[c, p, 1] = upper
                gain = own_gain[c, p]
                return (
                    gain * lower + z_recv[c, p, 0],
                    gain * upper + own_cross[c, p] * lower + z_recv[c, p, 1],
                )

            zero = jnp.zeros((block, width_y), jnp.float32)
            lax.fori_loop(0, slices, scan, (zero, zero), unroll=8)
            peers(lambda peer: r_copy(c, peer, place).start())
            r_recv[c, place] = r_send[c, place]

    def o_groups(c):
        return ((0, 3), (3, 5)) if c == chunks - 1 else ((0, 5),)

    def o_copy(c, group, peer, source):
        low, high = o_groups(c)[group]
        return pltpu.make_async_remote_copy(
            src_ref=o_send.at[c, peer, low:high],
            dst_ref=o_recv.at[c, source, low:high],
            send_sem=o_ss.at[c, group, peer],
            recv_sem=o_rs.at[c, group, source],
            device_id={"space": peer},
            device_id_type=MESH,
        )

    for c in range(chunks):
        owner_wait(r_recv.at[c], r_rs.at[c])
        own = hhat[c].reshape(owners, block, width_y)
        lower = jnp.where(place == 0, own, r_recv[c, :, 0]).reshape(length_z * rows, width_y)
        upper = jnp.where(place == 0, own, r_recv[c, :, 1]).reshape(length_z * rows, width_y)
        for m in range(5):
            if m == 0:
                value = upper
            else:
                value = (
                    gain_c[c, m - 1] * upper + gain_d[c, m - 1] * lower + part_b[c, m - 1]
                )
            planes = z_sine([value[k * rows : (k + 1) * rows] for k in range(length_z)])
            for z in range(length_z):
                o_send[c, z // depth, m, z % depth] = planes[z]
            o_recv[c, me, m] = o_send[c, me, m]
            for group, (_, high) in enumerate(o_groups(c)):
                if high == m + 1:
                    for i in range(1, spaces):
                        o_copy(c, group, lax.rem(me + i, spaces), me).start()

    for c in range(chunks):
        for i in range(1, spaces):
            peer = lax.rem(me + i, spaces)
            in_copy(c, 0, peer, me).wait_send()
            in_copy(c, 1, peer, me).wait_send()

        @pl.when(place == 0)
        def _():
            for i in range(1, spaces):
                in_copy(c, 2, lax.rem(me + i, spaces), me).wait_send()

        @pl.when(place < slices - 1)
        def _():
            h_copy(c, after).wait_send()

        owner_wait(z_send.at[c], z_ss.at[c])

        @pl.when(place < owners)
        def _():
            bulk_wait(r_send.at[c], r_ss.at[c], slices - 1)

    peers(lambda peer: step_copy(peer, place).wait_send())

    for m in range(5):
        for c in range(chunks):
            for group, (low, _) in enumerate(o_groups(c)):
                if low == m:
                    for i in range(1, spaces):
                        peer = lax.rem(me + i, spaces)
                        o_copy(c, group, peer, peer).wait_recv()
        field = jnp.stack(
            [
                jnp.concatenate(
                    [o_recv[c, s, m, z] for s in range(spaces) for c in range(chunks)], axis=0
                )
                for z in range(depth)
            ]
        )
        planes = lateral(field, x_pair, y_pair)
        for z in range(depth):
            result_ref[0, m, z] = planes[z]

    for c in range(chunks):
        for i in range(1, spaces):
            for group in range(len(o_groups(c))):
                o_copy(c, group, lax.rem(me + i, spaces), me).wait_send()


def body(initial, start_guess, forcing, step_size):
    depth, width_x, width_y = initial.shape
    spaces, slices = lax.axis_size("space"), lax.axis_size("tm")
    length_z = depth * spaces
    chunks = CHUNKS
    rows = width_x // spaces // chunks
    owners = min(slices, length_z * rows // 8)
    block = length_z * rows // owners
    dims = (spaces, slices, chunks, depth, length_z, rows, width_y, owners, block)

    def pair(length):
        full = jnp.asarray(sine(length), jnp.float32)
        return jnp.stack(split_pair(full))

    sides = jnp.asarray(eigen(width_x)[:, None] + eigen(width_y)[None, :], jnp.float32)
    f32 = jnp.float32
    flat = length_z * rows
    dma = pltpu.SemaphoreType.DMA
    vmem = pl.BlockSpec(memory_space=pltpu.VMEM)
    hbm = pl.BlockSpec(memory_space=pl.ANY)
    return pl.pallas_call(
        functools.partial(kernel, dims),
        out_shape=pltpu.VMEM((1, 5, depth, width_x, width_y), f32),
        in_specs=[pl.BlockSpec(memory_space=pltpu.SMEM), hbm, hbm, hbm, hbm, hbm, hbm],
        out_specs=vmem,
        scratch_shapes=[
            pltpu.VMEM((depth, width_x, width_y), f32),
            pltpu.VMEM((depth, width_x, width_y), f32),
            pltpu.VMEM((5, depth, width_x, width_y), f32),
            pltpu.VMEM((2, width_x, width_x), jnp.bfloat16),
            pltpu.VMEM((2, width_y, width_y), jnp.bfloat16),
            pltpu.VMEM((width_x, width_y), f32),
            pltpu.VMEM((chunks, spaces, 6, depth, rows, width_y), f32),
            pltpu.VMEM((chunks, spaces, 6, depth, rows, width_y), f32),
            pltpu.VMEM((chunks, flat, width_y), f32),
            pltpu.VMEM((chunks, flat, width_y), f32),
            pltpu.VMEM((chunks, flat, width_y), f32),
            pltpu.VMEM((8, width_y), f32),
            pltpu.VMEM((slices, 8, width_y), f32),
            pltpu.VMEM((chunks, 4, flat, width_y), f32),
            pltpu.VMEM((chunks, 4, flat, width_y), f32),
            pltpu.VMEM((chunks, 4, flat, width_y), f32),
            pltpu.VMEM((chunks, owners, 2, block, width_y), f32),
            pltpu.VMEM((chunks, slices, 2, block, width_y), f32),
            pltpu.VMEM((chunks, slices, block, width_y), f32),
            pltpu.VMEM((chunks, slices, block, width_y), f32),
            pltpu.VMEM((chunks, slices, 2, block, width_y), f32),
            pltpu.VMEM((chunks, owners, 2, block, width_y), f32),
            pltpu.VMEM((chunks, spaces, 5, depth, rows, width_y), f32),
            pltpu.VMEM((chunks, spaces, 5, depth, rows, width_y), f32),
            dma((6,)),
            dma((chunks, 3, spaces)),
            dma((chunks, 3, spaces)),
            dma((chunks,)),
            dma((chunks,)),
            dma((slices,)),
            dma((slices,)),
            dma((chunks,)),
            dma((chunks,)),
            dma((chunks,)),
            dma((chunks,)),
            dma((chunks, 5, spaces)),
            dma((chunks, 5, spaces)),
        ],
        compiler_params=pltpu.CompilerParams(collective_id=0, has_side_effects=True),
    )(step_size, initial, start_guess, forcing, pair(width_x), pair(width_y), sides)


def solution(mesh):
    in_specs = (
        P("space", None, None),
        P("tm", "space", None, None),
        P("tm", None, "space", None, None),
        P("tm"),
    )
    out_specs = P("tm", None, "space", None, None)
    return jax.shard_map(body, mesh=mesh, in_specs=in_specs, out_specs=out_specs, check_vma=False)
```

```python
import functools
import math

import jax
import jax.numpy as jnp
import numpy as np
from jax import lax
from jax.experimental import pallas as pl
from jax.experimental.pallas import tpu as pltpu
from jax.sharding import PartitionSpec as P

MESH = pl.DeviceIdType.MESH
CHUNKS = 2


def node_tables():
    radical = math.sqrt(3.0 / 7.0)
    node_times = [0.0, (1.0 - radical) / 2.0, 0.5, (1.0 + radical) / 2.0, 1.0]
    integrals = np.zeros((4, 5))
    for column in range(5):
        coeffs = [1.0]
        for other_index in range(5):
            if other_index == column:
                continue
            other_time = node_times[other_index]
            scaling = node_times[column] - other_time
            grown = [0.0] * (len(coeffs) + 1)
            for exponent in range(len(coeffs)):
                grown[exponent + 1] += coeffs[exponent] / scaling
                grown[exponent] -= coeffs[exponent] * other_time / scaling
            coeffs = grown
        for section in range(4):
            integrals[section, column] = sum(
                (
                    coeffs[exponent]
                    * (
                        node_times[section + 1] ** (exponent + 1)
                        - node_times[section] ** (exponent + 1)
                    )
                    / (exponent + 1)
                    for exponent in range(len(coeffs))
                )
            )
    coarse = [0.0, 0.5, 1.0]
    interp = np.zeros((5, 3))
    for column in range(3):
        for section in range(5):
            weight = 1.0
            for other_index in range(3):
                if other_index != column:
                    weight = (
                        weight
                        * (node_times[section] - coarse[other_index])
                        / (coarse[column] - coarse[other_index])
                    )
            interp[section, column] = weight
    return (np.array(node_times), integrals, interp)


def sine(length):
    k = np.arange(1, length + 1)
    phase = np.outer(k, k) % (2 * (length + 1))
    return math.sqrt(2.0 / (length + 1)) * np.sin(math.pi / (length + 1) * phase)


def eigen(length):
    return 2.0 - 2.0 * np.cos(math.pi / (length + 1) * np.arange(1, length + 1))


def split_pair(value):
    high = value.astype(jnp.bfloat16)
    return high, (value - high.astype(jnp.float32)).astype(jnp.bfloat16)


def dot(a, b):
    return jnp.dot(a, b, preferred_element_type=jnp.float32)


def precise(a, b):
    return dot(a[0], b[0]) + (dot(a[1], b[0]) + dot(a[0], b[1]))


def lateral(field, x_pair, y_pair):
    depth, width_x, width_y = field.shape
    mixed = precise(split_pair(field.reshape(depth * width_x, width_y)), y_pair)
    return [
        precise(x_pair, split_pair(mixed[z * width_x : (z + 1) * width_x])) for z in range(depth)
    ]


def z_sine(planes):
    count = len(planes)
    table = sine(count)
    half = (count + 1) // 2
    pairs = [
        (planes[z] + planes[count - 1 - z], planes[z] - planes[count - 1 - z])
        if z != count - 1 - z
        else (planes[z], None)
        for z in range(half)
    ]
    out = []
    for k in range(count):
        terms = [
            float(table[k, z]) * pairs[z][k % 2] for z in range(half) if pairs[z][k % 2] is not None
        ]
        total = terms[0]
        for term in terms[1:]:
            total = total + term
        out.append(total)
    return out


def weighted(weights, items):
    total = None
    for weight, item in zip(weights, items):
        weight = float(weight)
        if weight == 0.0 or item is None:
            continue
        term = item if weight == 1.0 else weight * item
        total = term if total is None else total + term
    return total


def sweep(rate, nodes, sources):
    times, integrals, _ = TABLES
    swept = [nodes[0]]
    for m in range(4):
        spacing = float(times[m + 1] - times[m])
        inner = weighted(integrals[m], nodes)
        if m > 0:
            inner = inner + spacing * (swept[m] - nodes[m])
        step = rate * inner
        if swept[m] is not None:
            step = step + swept[m]
        if sources is not None:
            step = step + sources[m]
        swept.append(step)
    first = list(integrals[0] + integrals[1])
    second = list(integrals[2] + integrals[3])
    first[0] -= 0.5
    second[2] -= 0.5
    left = rate * weighted(first, swept)
    right = rate * weighted(second, swept)
    if sources is not None:
        left = left + (sources[0] + sources[1])
        right = right + (sources[2] + sources[3])
    return swept, left, right


def corrected(swept, left, right, middle):
    interp = TABLES[2]
    ending = middle * left + right
    deltas = [None if swept[0] is None else -swept[0], left - swept[2], ending - swept[4]]
    return [
        None,
        swept[1] + weighted(interp[1], deltas),
        left,
        swept[3] + weighted(interp[3], deltas),
        ending,
    ]


def start_gains(middle):
    interp = TABLES[2]
    square = middle * middle
    return [
        None,
        float(interp[1, 0]) + float(interp[1, 1]) * middle + float(interp[1, 2]) * square,
        middle,
        float(interp[3, 0]) + float(interp[3, 1]) * middle + float(interp[3, 2]) * square,
        square,
    ]


def gains_of(rate):
    middle = 1.0 + 0.5 * rate
    gains = start_gains(middle)
    nodes = [jnp.ones_like(middle)] + gains[1:]
    swept, left, right = sweep(rate, nodes, None)
    return gains, corrected(swept, left, right, middle)


TABLES = node_tables()


def kernel(
    dims,
    step_ref, initial_hbm, guess_hbm, forcing_hbm, x_hbm, y_hbm, lateral_hbm,
    result_ref,
    initial, guess, forcing, x_ref, y_ref, lateral_ref,
    in_send, in_recv, ghat, hhat, ell, own_step, steps,
    gain_c, gain_d, part_b, z_send, z_recv, own_gain, own_cross, r_send, r_recv,
    o_send, o_recv,
    load_sem, in_ss, in_rs, h_ss, h_rs, s_ss, s_rs, z_ss, z_rs, r_ss, r_rs, o_ss, o_rs,
):
    spaces, slices, chunks, depth, length_z, rows, width_y, owners, block = dims
    me = lax.axis_index("space")
    place = lax.axis_index("tm")
    _, integrals, _ = TABLES
    width_x = spaces * chunks * rows

    barrier = pltpu.get_barrier_semaphore()
    for i in range(1, spaces):
        pl.semaphore_signal(
            barrier, inc=1, device_id={"space": lax.rem(me + i, spaces)}, device_id_type=MESH
        )

    def greet(i, carry):
        pl.semaphore_signal(
            barrier, inc=1, device_id={"tm": lax.rem(place + i, slices)}, device_id_type=MESH
        )
        return carry

    lax.fori_loop(1, slices, greet, 0)

    sources = (guess_hbm.at[0], x_hbm, y_hbm, forcing_hbm.at[0], initial_hbm, lateral_hbm)
    loads = [
        pltpu.make_async_copy(source, target, load_sem.at[i])
        for i, (source, target) in enumerate(
            zip(sources, (guess, x_ref, y_ref, forcing, initial, lateral_ref))
        )
    ]
    for load in loads:
        load.start()
    load_guess, load_x, load_y, load_forcing, load_initial, load_lateral = loads

    step = step_ref[0]
    own_step[...] = jnp.full(own_step.shape, step, jnp.float32)
    steps[place] = jnp.full(own_step.shape, step, jnp.float32)

    def put(field, slot):
        planes = lateral(field, x_pair, y_pair)
        for target in range(spaces):
            for c in range(chunks):
                low = (target * chunks + c) * rows
                for z in range(depth):
                    in_send[c, target, slot, z] = planes[z][low : low + rows]

    def keep(c, low, high):
        in_recv[c, me, low:high] = in_send[c, me, low:high]

    groups = ((0, 1), (1, 5), (5, 6))

    def in_copy(c, group, peer, source):
        low, high = groups[group]
        return pltpu.make_async_remote_copy(
            src_ref=in_send.at[c, peer, low:high],
            dst_ref=in_recv.at[c, source, low:high],
            send_sem=in_ss.at[c, group, peer],
            recv_sem=in_rs.at[c, group, source],
            device_id={"space": peer},
            device_id_type=MESH,
        )

    def in_start(c, group):
        for i in range(1, spaces):
            in_copy(c, group, lax.rem(me + i, spaces), me).start()

    def in_wait(c, group):
        for i in range(1, spaces):
            peer = lax.rem(me + i, spaces)
            in_copy(c, group, peer, peer).wait_recv()

    load_guess.wait()
    load_x.wait()
    load_y.wait()
    x_pair = (x_ref[0], x_ref[1])
    y_pair = (y_ref[0], y_ref[1])
    put(guess[...], 0)
    pl.semaphore_wait(barrier, spaces - 1 + slices - 1)
    for c in range(chunks):
        in_start(c, 0)

    def step_copy(peer, source):
        return pltpu.make_async_remote_copy(
            src_ref=own_step,
            dst_ref=steps.at[source],
            send_sem=s_ss.at[peer],
            recv_sem=s_rs.at[source],
            device_id={"tm": peer},
            device_id_type=MESH,
        )

    def peers(action):
        def one(i, carry):
            action(lax.rem(place + i, slices))
            return carry

        if slices > 8:
            lax.fori_loop(1, slices, one, 0)
        else:
            for i in range(1, slices):
                one(i, 0)


    for c in range(chunks):
        keep(c, 0, 1)
    load_initial.wait()

    @pl.when(place == 0)
    def _():
        put(initial[...], 5)
        for c in range(chunks):
            in_start(c, 2)
            keep(c, 5, 6)

    load_forcing.wait()
    for m in range(4):
        put(step * weighted(integrals[m], [forcing[j] for j in range(5)]), m + 1)
    for c in range(chunks):
        in_start(c, 1)
        keep(c, 1, 5)
    peers(lambda peer: step_copy(peer, place).start())

    z_eigen = eigen(length_z)
    load_lateral.wait()
    for c in range(chunks):
        low = pl.multiple_of((me * chunks + c) * rows, 8)
        base = lateral_ref[pl.ds(low, rows), :]
        for k in range(length_z):
            ell[c, k * rows : (k + 1) * rows] = -(base + float(z_eigen[k]))

    def table(i, carry):
        for c in range(chunks):
            at = pl.ds(pl.multiple_of(i * rows, 8), rows)
            gains, crossed = gains_of(step * ell[c, at])
            for m in range(1, 5):
                gain_c[c, m - 1, at] = gains[m]
                gain_d[c, m - 1, at] = crossed[m]
        return carry

    lax.fori_loop(0, length_z, table, 0, unroll=2)

    def planes_of(c, slot):
        return [in_recv[c, z // depth, slot, z % depth] for z in range(length_z)]

    def h_copy(c, peer):
        return pltpu.make_async_remote_copy(
            src_ref=ghat.at[c],
            dst_ref=hhat.at[c],
            send_sem=h_ss.at[c],
            recv_sem=h_rs.at[c],
            device_id={"tm": peer},
            device_id_type=MESH,
        )

    after = lax.rem(place + 1, slices)
    for c in range(chunks):
        in_wait(c, 0)
        for k, plane in enumerate(z_sine(planes_of(c, 0))):
            ghat[c, k * rows : (k + 1) * rows] = plane

        @pl.when(place < slices - 1)
        def _():
            h_copy(c, after).start()

    peers(lambda peer: step_copy(peer, peer).wait_recv())

    @pl.when(place < owners)
    def _():
        def one(p, carry):
            for c in range(chunks):
                at = pl.ds(pl.multiple_of(place * block, 8), block)
                gains, crossed = gains_of(steps[p][0:1] * ell[c, at])
                own_gain[c, p] = gains[4]
                own_cross[c, p] = crossed[4]
            return carry

        lax.fori_loop(0, slices, one, 0, unroll=2)

    def z_copy(c, owner, source):
        return pltpu.make_async_remote_copy(
            src_ref=z_send.at[c, owner],
            dst_ref=z_recv.at[c, source],
            send_sem=z_ss.at[c],
            recv_sem=z_rs.at[c],
            device_id={"tm": owner},
            device_id_type=MESH,
        )

    def to_owner(owner, action):
        if owners == slices:
            action()
        else:
            pl.when(owner < owners)(action)

    def bulk_wait(ref, sem, count):
        pltpu.make_async_copy(ref.at[0:count], ref.at[0:count], sem).wait()

    def owner_wait(ref, sem):
        if owners == slices:
            bulk_wait(ref, sem, owners - 1)
        else:
            pl.when(place < owners)(lambda: bulk_wait(ref, sem, owners - 1))
            pl.when(place >= owners)(lambda: bulk_wait(ref, sem, owners))

    first = jnp.where(place == 0, 1.0, 0.0).astype(jnp.float32)
    for c in range(chunks):
        in_wait(c, 1)
        fhat = [z_sine(planes_of(c, m + 1)) for m in range(4)]
        for m in range(4):
            for k in range(length_z):
                part_b[c, m, k * rows : (k + 1) * rows] = fhat[m][k]

        @pl.when(place == 0)
        def _():
            in_wait(c, 2)
            for k, plane in enumerate(z_sine(planes_of(c, 5))):
                hhat[c, k * rows : (k + 1) * rows] = plane

        @pl.when(place > 0)
        def _():
            h_copy(c, after).wait_recv()

        def solve(i, carry):
            at = pl.ds(pl.multiple_of(i * block, 8), block)
            rate = step * ell[c, at]
            middle = 1.0 + 0.5 * rate
            guess_hat, start = ghat[c, at], hhat[c, at]
            sources = [part_b[c, m, at] for m in range(4)]
            one = sweep(rate, [start] + [guess_hat] * 4, sources)
            nodes = corrected(*one, middle)
            rest = corrected(*sweep(rate, nodes, sources), middle)
            for m in range(1, 5):
                part_b[c, m - 1, at] = rest[m]
            seen = first * start
            gain, cross = gain_c[c, 3, at], gain_d[c, 3, at]
            z_send[c, i, 0] = nodes[4] + gain * seen
            z_send[c, i, 1] = rest[4] + (gain + cross) * seen
            return carry

        lax.fori_loop(0, owners, solve, 0, unroll=4)
        peers(lambda peer: to_owner(peer, lambda: z_copy(c, peer, place).start()))

        @pl.when(place < owners)
        def _():
            z_recv[c, place] = z_send[c, place]

    def r_copy(c, target, owner):
        return pltpu.make_async_remote_copy(
            src_ref=r_send.at[c, target],
            dst_ref=r_recv.at[c, owner],
            send_sem=r_ss.at[c],
            recv_sem=r_rs.at[c],
            device_id={"tm": target},
            device_id_type=MESH,
        )

    for c in range(chunks):
        @pl.when(place < owners)
        def _():
            bulk_wait(z_recv.at[c], z_rs.at[c], slices - 1)

            def scan(p, state):
                lower, upper = state
                r_send[c, p, 0] = lower
                r_send[c, p, 1] = upper
                gain = own_gain[c, p]
                return (
                    gain * lower + z_recv[c, p, 0],
                    gain * upper + own_cross[c, p] * lower + z_recv[c, p, 1],
                )

            zero = jnp.zeros((block, width_y), jnp.float32)
            lax.fori_loop(0, slices, scan, (zero, zero), unroll=8)
            peers(lambda peer: r_copy(c, peer, place).start())
            r_recv[c, place] = r_send[c, place]

    def o_groups(c):
        return ((0, 3), (3, 5)) if c == chunks - 1 else ((0, 5),)

    def o_copy(c, group, peer, source):
        low, high = o_groups(c)[group]
        return pltpu.make_async_remote_copy(
            src_ref=o_send.at[c, peer, low:high],
            dst_ref=o_recv.at[c, source, low:high],
            send_sem=o_ss.at[c, group, peer],
            recv_sem=o_rs.at[c, group, source],
            device_id={"space": peer},
            device_id_type=MESH,
        )

    for c in range(chunks):
        owner_wait(r_recv.at[c], r_rs.at[c])
        own = hhat[c].reshape(owners, block, width_y)
        lower = jnp.where(place == 0, own, r_recv[c, :, 0]).reshape(length_z * rows, width_y)
        upper = jnp.where(place == 0, own, r_recv[c, :, 1]).reshape(length_z * rows, width_y)
        for m in range(5):
            if m == 0:
                value = upper
            else:
                value = (
                    gain_c[c, m - 1] * upper + gain_d[c, m - 1] * lower + part_b[c, m - 1]
                )
            planes = z_sine([value[k * rows : (k + 1) * rows] for k in range(length_z)])
            for z in range(length_z):
                o_send[c, z // depth, m, z % depth] = planes[z]
            for group, (_, high) in enumerate(o_groups(c)):
                if high == m + 1:
                    for i in range(1, spaces):
                        o_copy(c, group, lax.rem(me + i, spaces), me).start()
            o_recv[c, me, m] = o_send[c, me, m]

    for c in range(chunks):
        for i in range(1, spaces):
            peer = lax.rem(me + i, spaces)
            in_copy(c, 0, peer, me).wait_send()
            in_copy(c, 1, peer, me).wait_send()

        @pl.when(place == 0)
        def _():
            for i in range(1, spaces):
                in_copy(c, 2, lax.rem(me + i, spaces), me).wait_send()

        @pl.when(place < slices - 1)
        def _():
            h_copy(c, after).wait_send()

        owner_wait(z_send.at[c], z_ss.at[c])

        @pl.when(place < owners)
        def _():
            bulk_wait(r_send.at[c], r_ss.at[c], slices - 1)

    peers(lambda peer: step_copy(peer, place).wait_send())

    for m in range(5):
        for c in range(chunks):
            for group, (low, _) in enumerate(o_groups(c)):
                if low == m:
                    for i in range(1, spaces):
                        peer = lax.rem(me + i, spaces)
                        o_copy(c, group, peer, peer).wait_recv()
        field = jnp.stack(
            [
                jnp.concatenate(
                    [o_recv[c, s, m, z] for s in range(spaces) for c in range(chunks)], axis=0
                )
                for z in range(depth)
            ]
        )
        planes = lateral(field, x_pair, y_pair)
        for z in range(depth):
            result_ref[0, m, z] = planes[z]

    for c in range(chunks):
        for i in range(1, spaces):
            for group in range(len(o_groups(c))):
                o_copy(c, group, lax.rem(me + i, spaces), me).wait_send()


def body(initial, start_guess, forcing, step_size):
    depth, width_x, width_y = initial.shape
    spaces, slices = lax.axis_size("space"), lax.axis_size("tm")
    length_z = depth * spaces
    chunks = CHUNKS
    rows = width_x // spaces // chunks
    owners = min(slices, length_z * rows // 8)
    block = length_z * rows // owners
    dims = (spaces, slices, chunks, depth, length_z, rows, width_y, owners, block)

    def pair(length):
        full = jnp.asarray(sine(length), jnp.float32)
        return jnp.stack(split_pair(full))

    sides = jnp.asarray(eigen(width_x)[:, None] + eigen(width_y)[None, :], jnp.float32)
    f32 = jnp.float32
    flat = length_z * rows
    dma = pltpu.SemaphoreType.DMA
    vmem = pl.BlockSpec(memory_space=pltpu.VMEM)
    hbm = pl.BlockSpec(memory_space=pl.ANY)
    return pl.pallas_call(
        functools.partial(kernel, dims),
        out_shape=pltpu.VMEM((1, 5, depth, width_x, width_y), f32),
        in_specs=[pl.BlockSpec(memory_space=pltpu.SMEM), hbm, hbm, hbm, hbm, hbm, hbm],
        out_specs=vmem,
        scratch_shapes=[
            pltpu.VMEM((depth, width_x, width_y), f32),
            pltpu.VMEM((depth, width_x, width_y), f32),
            pltpu.VMEM((5, depth, width_x, width_y), f32),
            pltpu.VMEM((2, width_x, width_x), jnp.bfloat16),
            pltpu.VMEM((2, width_y, width_y), jnp.bfloat16),
            pltpu.VMEM((width_x, width_y), f32),
            pltpu.VMEM((chunks, spaces, 6, depth, rows, width_y), f32),
            pltpu.VMEM((chunks, spaces, 6, depth, rows, width_y), f32),
            pltpu.VMEM((chunks, flat, width_y), f32),
            pltpu.VMEM((chunks, flat, width_y), f32),
            pltpu.VMEM((chunks, flat, width_y), f32),
            pltpu.VMEM((8, width_y), f32),
            pltpu.VMEM((slices, 8, width_y), f32),
            pltpu.VMEM((chunks, 4, flat, width_y), f32),
            pltpu.VMEM((chunks, 4, flat, width_y), f32),
            pltpu.VMEM((chunks, 4, flat, width_y), f32),
            pltpu.VMEM((chunks, owners, 2, block, width_y), f32),
            pltpu.VMEM((chunks, slices, 2, block, width_y), f32),
            pltpu.VMEM((chunks, slices, block, width_y), f32),
            pltpu.VMEM((chunks, slices, block, width_y), f32),
            pltpu.VMEM((chunks, slices, 2, block, width_y), f32),
            pltpu.VMEM((chunks, owners, 2, block, width_y), f32),
            pltpu.VMEM((chunks, spaces, 5, depth, rows, width_y), f32),
            pltpu.VMEM((chunks, spaces, 5, depth, rows, width_y), f32),
            dma((6,)),
            dma((chunks, 3, spaces)),
            dma((chunks, 3, spaces)),
            dma((chunks,)),
            dma((chunks,)),
            dma((slices,)),
            dma((slices,)),
            dma((chunks,)),
            dma((chunks,)),
            dma((chunks,)),
            dma((chunks,)),
            dma((chunks, 5, spaces)),
            dma((chunks, 5, spaces)),
        ],
        compiler_params=pltpu.CompilerParams(collective_id=0, has_side_effects=True),
    )(step_size, initial, start_guess, forcing, pair(width_x), pair(width_y), sides)


def solution(mesh):
    in_specs = (
        P("space", None, None),
        P("tm", "space", None, None),
        P("tm", None, "space", None, None),
        P("tm"),
    )
    out_specs = P("tm", None, "space", None, None)
    return jax.shard_map(body, mesh=mesh, in_specs=in_specs, out_specs=out_specs, check_vma=False)
```
